256 devices in a mesh: bank: 16 (over z, core), zero: 16 (over y, x).
Axes of the slice: x: 4, y: 4, z: 8, core: 2. Of those that a mesh axis runs over, the one named last changes fastest.
Arguments:
- master_gate: float32 [64, 2048, 1408], P('bank', 'zero'), may hold values from -0.1875 to 0.1875
- master_up: float32 [64, 2048, 1408], P('bank', 'zero'), may hold values from -0.1875 to 0.1875
- master_down: float32 [64, 1408, 2048], P('bank', None, 'zero'), may hold values from -0.21875 to 0.21875
- router_weight: float32 [2048, 64], P('zero', 'bank'), may hold values from -0.125 to 0.125
- router_gain: float32 [2048], P('zero'), may hold values from 0.25 to 1.75
Outputs:
- final_gate: bfloat16 [64, 2048, 1408], P('bank', None, 'zero')
- final_up: bfloat16 [64, 2048, 1408], P('bank', None, 'zero')
- final_down: bfloat16 [64, 1408, 2048], P('bank', 'zero')
- scale_gate: float32 [64, 1408], P('bank', 'zero')
- scale_up: float32 [64, 1408], P('bank', 'zero')
- scale_down: float32 [64, 1408], P('bank', 'zero')
- serve_router: bfloat16 [2048, 64], replicated
The draws below stay inside these ranges and needn't reach their ends.
All inputs are finite; a program needn't handle non-finite values. Where the reference program divides by a largest or mean magnitude, that divisor is 1e-20 or more.
Results may differ from the reference program's by a relative error of at most 0.0013.
Values may be sent and summed in bfloat16 or wider, within the bound.
A program may use at most 64 MiB of HBM per device.

```python
import jax
import jax.numpy as jnp

EXPERTS = 64
D_MODEL = 2048
D_EXPERT = 1408


def strengthened(drawn, key, source, target, blocks, factor):
    owner, partner = [(jnp.arange(drawn.shape[axis_at]) // (drawn.shape[axis_at] // blocks)).reshape([-1 if axis == axis_at else 1 for axis in range(drawn.ndim)]) for axis_at in (source, target)]
    chosen = jax.random.permutation(key, blocks)[partner]
    strong = (owner == chosen) | (owner == (partner + blocks // 2) % blocks)
    return jnp.where(strong, factor * drawn, drawn)


def level_of(rng, extent, split, least, high):
    def one(position, parts):
        steps = jax.random.uniform(jax.random.fold_in(jax.random.fold_in(rng, 6), position), (parts,), jnp.float32, least / len(split), high / len(split))
        return jnp.repeat(jnp.exp(steps), extent[position] // parts).reshape((-1,) + (1,) * (len(extent) - position - 1))

    loudness = one(*split[0])
    for cut in split[1:]:
        loudness = loudness * one(*cut)
    return loudness


def normal_values(own_key, dims, width, reach, cuts=(), held_as=jnp.bfloat16):
    values = width * jax.random.normal(own_key, dims, jnp.float32)
    if cuts:
        values = values * level_of(own_key, dims, cuts, -0.22, 0.18)
    return jnp.clip(values, -reach, reach).astype(held_as)


def noise_with(own_key, extent, scale, reach, pieces, heavy, dtype=jnp.bfloat16):
    entries = scale * jax.random.normal(own_key, extent, jnp.float32)
    if pieces:
        entries = entries * level_of(own_key, extent, pieces, -0.22, 0.18)
    return jnp.clip(strengthened(entries, jax.random.fold_in(own_key, 3), *heavy), -reach, reach).astype(dtype)


def setup_inputs(seed: int = 0) -> dict:
    keys = jax.random.split(jax.random.key(seed), 6)
    return {
        "master_gate": noise_with(keys[0], (EXPERTS, D_MODEL, D_EXPERT), D_MODEL ** -0.5, 0.1875, ((0, 16), (1, 16)), (1, 2, 16, 2.0), jnp.float32),
        "master_up": noise_with(keys[1], (EXPERTS, D_MODEL, D_EXPERT), D_MODEL ** -0.5, 0.1875, ((0, 16), (1, 16)), (1, 2, 16, 2.0), jnp.float32),
        "master_down": noise_with(keys[2], (EXPERTS, D_EXPERT, D_MODEL), D_EXPERT ** -0.5, 0.21875, ((0, 16), (2, 16)), (2, 1, 16, 2.0), jnp.float32),
        "router_weight": normal_values(keys[3], (D_MODEL, EXPERTS), D_MODEL ** -0.5, 0.125, ((0, 16), (1, 16)), jnp.float32),
        "router_gain": jnp.clip(1.0 + 0.15 * jax.random.normal(keys[4], (D_MODEL,), jnp.float32), 0.25, 1.75),
    }


def reference(master_gate, master_up, master_down, router_weight, router_gain):
    scale_gate = jnp.sum(jnp.abs(master_gate), axis=1) / D_MODEL
    final_gate = (master_gate / jnp.expand_dims(scale_gate, 1)).astype(jnp.bfloat16)
    scale_up = jnp.sum(jnp.abs(master_up), axis=1) / D_MODEL
    final_up = (master_up / jnp.expand_dims(scale_up, 1)).astype(jnp.bfloat16)
    scale_down = jnp.sum(jnp.abs(master_down), axis=2) / D_MODEL
    final_down = (master_down / jnp.expand_dims(scale_down, 2)).astype(jnp.bfloat16)
    serve_router = (router_weight * router_gain[:, None]).astype(jnp.bfloat16)
    return final_gate, final_up, final_down, scale_gate, scale_up, scale_down, serve_router
```

```python
import functools

import jax
import jax.numpy as jnp
from jax import lax
from jax.experimental import pallas as pl
from jax.experimental.pallas import tpu as pltpu
from jax.sharding import PartitionSpec as P

MESH = pl.DeviceIdType.MESH
N = 16
D_MODEL = 2048
EXP = 4
WIDE = 1408
OWN = 128
PIECE = WIDE // N


def exchange_kernel(
    gate, up, down, weight, gain,
    out_gate, out_up, out_down, scales_ab, scales_c, router_rows,
    x, t, s, piece_a, piece_b, part_a, part_b, mine_a, mine_b, all_a, all_b,
    send, router_part, router_line,
    load_sem, rs_send, rs_recv, ag_send, ag_recv, out_send, out_recv, rz_send, rz_recv, rb_send, rb_recv,
):
    me = lax.axis_index("zero")
    bank = lax.axis_index("bank")

    def peer(k):
        y, xx = me // 4, me % 4
        return ((y + k // 4) % 4) * 4 + (xx + k % 4) % 4

    def bank_peer(k):
        return ((bank // 2 + k // 2) % 8) * 2 + (bank % 2 + k % 2) % 2

    def remote(src, dst, send_sem, recv_sem, to):
        return pltpu.make_async_remote_copy(
            src_ref=src, dst_ref=dst, send_sem=send_sem, recv_sem=recv_sem, device_id=to, device_id_type=MESH
        )

    loads = []
    for m in range(12):
        source = (gate, up, down)[m // 4].at[m % 4]
        target = x.at[m] if m < 8 else t.at[m]
        loads.append(pltpu.make_async_copy(source, target, load_sem.at[m]))
    for c in loads:
        c.start()

    barrier = pltpu.get_barrier_semaphore()

    @pl.loop(1, N)
    def _(k):
        pl.semaphore_signal(barrier, inc=1, device_id=(bank, peer(k)), device_id_type=MESH)
        pl.semaphore_signal(barrier, inc=1, device_id=(bank_peer(k), me), device_id_type=MESH)

    router_part[...] = (weight[...] * gain[...]).astype(jnp.bfloat16)
    column = pl.ds(pl.multiple_of(me * OWN, OWN), OWN)
    router_line[:, column] = router_part[...]

    for m in range(8):
        loads[m].wait()
        s[pl.ds(m, 1), pl.ds(0, WIDE)] = jnp.sum(jnp.abs(x[m]), axis=0, keepdims=True)
    s[:, pl.ds(WIDE, 128)] = jnp.zeros((8, 128), jnp.float32)
    for d in range(N):
        base = (PIECE * d) // 128 * 128
        both = s[:, pl.ds(base, 256)]
        shift = (256 - (PIECE * d - base)) % 256
        piece_a[d] = (pltpu.roll(both, shift, 1) if shift else both)[:, :128]
    pl.semaphore_wait(barrier, 2 * (N - 1))

    def rs_copy(k, piece, part, which):
        to = peer(k)
        return remote(piece.at[to], part.at[me], rs_send.at[which, k], rs_recv.at[which, k], (bank, to))

    def rz_copy(k):
        return remote(router_part, router_line.at[:, column], rz_send.at[k], rz_recv.at[k], (bank, peer(k)))

    @pl.loop(1, N)
    def _(k):
        rs_copy(k, piece_a, part_a, 0).start()

    part_a[me] = piece_a[me]

    eye = lax.broadcasted_iota(jnp.int32, (PIECE, OWN), 0) == lax.broadcasted_iota(jnp.int32, (PIECE, OWN), 1)
    for m in range(8, 12):
        loads[m].wait()

    @pl.loop(0, N)
    def _(d):
        rows = pl.ds(pl.multiple_of(d * PIECE, 8), PIECE)
        for e in range(EXP):
            total = jnp.sum(jnp.abs(t[8 + e, rows, :]), axis=1, keepdims=True)
            piece_b[d, pl.ds(e, 1), :] = jnp.sum(jnp.where(eye, total, 0.0), axis=0, keepdims=True)
        piece_b[d, pl.ds(4, 4), :] = jnp.zeros((4, OWN), jnp.float32)

    @pl.loop(1, N)
    def _(k):
        rs_copy(k, piece_b, part_b, 1).start()
        rz_copy(k).start()

    part_b[me] = piece_b[me]

    def turn(lo, hi):
        for m in range(lo, hi):
            for c in range(WIDE // 128):
                t[m, pl.ds(c * 128, 128), :] = x[m, :, pl.ds(c * 128, 128)].T

    def ag_copy(k, mine, whole, which):
        return remote(mine, whole.at[me], ag_send.at[which, k], ag_recv.at[which, k], (bank, peer(k)))

    def reduce_and_spread(piece, part, mine, whole, which):
        @pl.loop(1, N)
        def _(k):
            rs_copy(k, piece, part, which).wait_recv()

        total = part[0]
        for d in range(1, N):
            total = total + part[d]
        scale = total / D_MODEL
        mine[...] = scale
        whole[me] = scale

        @pl.loop(1, N)
        def _(k):
            ag_copy(k, mine, whole, which).start()

        return scale

    turn(0, 4)
    scale_a = reduce_and_spread(piece_a, part_a, mine_a, all_a, 0)
    scales_ab[...] = scale_a
    scale_b = reduce_and_spread(piece_b, part_b, mine_b, all_b, 1)
    scales_c[...] = scale_b

    @pl.loop(1, N)
    def _(k):
        rz_copy(k).wait_recv()

    def rb_copy(k):
        return remote(router_line, router_rows.at[bank], rb_send.at[k], rb_recv.at[k], (bank_peer(k), me))

    @pl.loop(1, N)
    def _(k):
        rb_copy(k).start()

    router_rows[bank] = router_line[...]

    turn(4, 8)

    @pl.loop(1, N)
    def _(k):
        ag_copy(k, mine_a, all_a, 0).wait_recv()
        ag_copy(k, mine_b, all_b, 1).wait_recv()

    outs = (out_gate, out_up, out_down)

    def scaled(to, m):
        row = (all_a if m < 8 else all_b)[to, pl.ds(m % 8, 1), :]
        factor = jnp.sum(jnp.where(eye, 1.0 / row, 0.0), axis=1, keepdims=True)
        rows = pl.ds(pl.multiple_of(to * PIECE, 8), PIECE)
        return (t[m, rows, :] * factor).astype(jnp.bfloat16)

    def out_copy(k, i):
        return remote(
            send.at[k, pl.ds(4 * i, 4)], outs[i].at[:, :, column], out_send.at[i, k], out_recv.at[i, k], (bank, peer(k))
        )

    @pl.loop(1, N)
    def _(k):
        to = peer(k)
        for i in range(3):
            for e in range(EXP):
                send[k, 4 * i + e] = scaled(to, 4 * i + e)
            out_copy(k, i).start()

    for m in range(12):
        outs[m // 4][m % 4, :, column] = scaled(me, m)

    @pl.loop(1, N)
    def _(k):
        for i in range(3):
            out_copy(k, i).wait()
        rb_copy(k).wait()
        rz_copy(k).wait_send()
        for which, (piece, part, mine, whole) in enumerate(
            ((piece_a, part_a, mine_a, all_a), (piece_b, part_b, mine_b, all_b))
        ):
            rs_copy(k, piece, part, which).wait_send()
            ag_copy(k, mine, whole, which).wait_send()


def exchange(gate, up, down, weight, gain):
    f32, bf16 = jnp.float32, jnp.bfloat16
    vmem, anywhere = pl.BlockSpec(memory_space=pltpu.VMEM), pl.BlockSpec(memory_space=pl.ANY)
    big = jax.ShapeDtypeStruct((EXP, PIECE, D_MODEL), bf16)
    small = jax.ShapeDtypeStruct((8, 128), f32)
    return pl.pallas_call(
        exchange_kernel,
        name="exchange",
        out_shape=(big, big, big, small, small, jax.ShapeDtypeStruct((N, EXP, D_MODEL), bf16)),
        in_specs=[anywhere, anywhere, anywhere, vmem, vmem],
        out_specs=(vmem,) * 6,
        scratch_shapes=[
            pltpu.VMEM((8, OWN, WIDE), f32),
            pltpu.VMEM((12, WIDE, OWN), f32),
            pltpu.VMEM((8, WIDE + 128), f32),
            pltpu.VMEM((N, 8, 128), f32),
            pltpu.VMEM((N, 8, 128), f32),
            pltpu.VMEM((N, 8, 128), f32),
            pltpu.VMEM((N, 8, 128), f32),
            pltpu.VMEM((8, 128), f32),
            pltpu.VMEM((8, 128), f32),
            pltpu.VMEM((N, 8, 128), f32),
            pltpu.VMEM((N, 8, 128), f32),
            pltpu.VMEM((N, 12, PIECE, OWN), bf16),
            pltpu.VMEM((EXP, OWN), bf16),
            pltpu.VMEM((EXP, D_MODEL), bf16),
            pltpu.SemaphoreType.DMA((12,)),
            pltpu.SemaphoreType.DMA((2, N)),
            pltpu.SemaphoreType.DMA((2, N)),
            pltpu.SemaphoreType.DMA((2, N)),
            pltpu.SemaphoreType.DMA((2, N)),
            pltpu.SemaphoreType.DMA((3, N)),
            pltpu.SemaphoreType.DMA((3, N)),
            pltpu.SemaphoreType.DMA((N,)),
            pltpu.SemaphoreType.DMA((N,)),
            pltpu.SemaphoreType.DMA((N,)),
            pltpu.SemaphoreType.DMA((N,)),
        ],
        compiler_params=pltpu.CompilerParams(
            collective_id=0, has_side_effects=True, vmem_limit_bytes=48 * 1024 * 1024
        ),
    )(gate, up, down, weight, gain)


def finish_kernel(a, b, c, scales_ab, scales_c, rows, fa, fb, fc, sa, sb, sc, fr, router, sem):
    copies = [
        pltpu.make_async_copy(src, dst, sem.at[i]) for i, (src, dst) in enumerate(((a, fa), (b, fb), (c, fc)))
    ]
    for c_ in copies:
        c_.start()
    sa[...] = scales_ab[pl.ds(0, 4), pl.ds(0, PIECE)]
    sb[...] = scales_ab[pl.ds(4, 4), pl.ds(0, PIECE)]
    sc[...] = scales_c[pl.ds(0, 4), pl.ds(0, PIECE)]
    for i in range(N):
        router[pl.ds(4 * i, 4), :] = rows[i]
    last = pltpu.make_async_copy(router, fr, sem.at[3])
    last.start()
    for c_ in copies:
        c_.wait()
    last.wait()


def finish(*parts):
    f32, bf16 = jnp.float32, jnp.bfloat16
    vmem, anywhere = pl.BlockSpec(memory_space=pltpu.VMEM), pl.BlockSpec(memory_space=pl.ANY)
    big = jax.ShapeDtypeStruct((EXP, PIECE, D_MODEL), bf16)
    small = jax.ShapeDtypeStruct((EXP, PIECE), f32)
    return pl.pallas_call(
        finish_kernel,
        name="finish",
        out_shape=(big, big, big, small, small, small, jax.ShapeDtypeStruct((N * EXP, D_MODEL), bf16)),
        in_specs=[vmem] * 6,
        out_specs=(anywhere,) * 3 + (vmem,) * 3 + (anywhere,),
        scratch_shapes=[pltpu.VMEM((N * EXP, D_MODEL), bf16), pltpu.SemaphoreType.DMA((4,))],
        compiler_params=pltpu.CompilerParams(vmem_limit_bytes=16 * 1024 * 1024),
    )(*parts)


def local(master_gate, master_up, master_down, router_weight, router_gain):
    parts = exchange(master_gate, master_up, master_down, router_weight.T, router_gain.reshape(1, OWN))
    fa, fb, fc, sa, sb, sc, fr = finish(*parts)
    return (fa.transpose(0, 2, 1), fb.transpose(0, 2, 1), fc, sa, sb, sc, fr.T)


def solution(mesh):
    placed = (
        P("bank", "zero", None),
        P("bank", "zero", None),
        P("bank", None, "zero"),
        P("zero", "bank"),
        P("zero"),
    )
    return jax.shard_map(
        local,
        mesh=mesh,
        in_specs=placed,
        out_specs=(
            P("bank", None, "zero"),
            P("bank", None, "zero"),
            P("bank", "zero", None),
            P("bank", "zero"),
            P("bank", "zero"),
            P("bank", "zero"),
            P(),
        ),
        check_vma=False,
    )
```

```python
import functools

import jax
import jax.numpy as jnp
from jax import lax
from jax.experimental import pallas as pl
from jax.experimental.pallas import tpu as pltpu
from jax.sharding import PartitionSpec as P

MESH = pl.DeviceIdType.MESH
N = 16
D_MODEL = 2048
EXP = 4
WIDE = 1408
OWN = 128
PIECE = WIDE // N
PEERS = ((1, 1), (3, 3), (1, 3), (3, 1), (1, 0), (3, 0), (0, 1), (0, 3), (1, 2), (3, 2), (2, 1), (2, 3), (2, 2), (0, 2), (2, 0))
ORDER = tuple(4 * a + b for a, b in PEERS)


def exchange_kernel(
    gate, up, down, weight_hbm, gain_hbm,
    out_gate, out_up, out_down, scales_ab, scales_c, router_rows,
    x, t, s, piece_a, piece_b, part_a, part_b, mine_a, mine_b, all_a, all_b,
    send, router_part, router_line, weight, gain,
    load_sem, rs_send, rs_recv, ag_send, ag_recv, out_send, out_recv, rz_send, rz_recv, rb_send, rb_recv, later,
):
    me = lax.axis_index("zero")
    bank = lax.axis_index("bank")

    def peer(k):
        y, xx = me // 4, me % 4
        return ((y + k // 4) % 4) * 4 + (xx + k % 4) % 4

    def bank_peer(k):
        return (bank + k) % N

    def remote(src, dst, send_sem, recv_sem, to):
        return pltpu.make_async_remote_copy(
            src_ref=src, dst_ref=dst, send_sem=send_sem, recv_sem=recv_sem, device_id=to, device_id_type=MESH
        )

    column = pl.ds(pl.multiple_of(me * OWN, OWN), OWN)
    loads = []
    for m in range(12):
        source = (gate, up, down)[m // 4].at[m % 4]
        target = x.at[m] if m < 8 else t.at[m]
        loads.append(pltpu.make_async_copy(source, target, load_sem.at[m]))
    for c in loads:
        c.start()

    barrier = pltpu.get_barrier_semaphore()

    for k in ORDER:
        pl.semaphore_signal(barrier, inc=1, device_id=(bank, peer(k)), device_id_type=MESH)

    @pl.loop(1, N)
    def _(j):
        @pl.when(bank + j < N)
        def _():
            pl.semaphore_signal(barrier, inc=1, device_id=(bank + j, me), device_id_type=MESH)

    small_loads = [
        pltpu.make_async_copy(weight_hbm, weight, load_sem.at[12]),
        pltpu.make_async_copy(gain_hbm, gain, load_sem.at[13]),
    ]
    for c in small_loads:
        c.start()
    for m in range(8):
        loads[m].wait()
        s[pl.ds(m, 1), pl.ds(0, WIDE)] = jnp.sum(jnp.abs(x[m]), axis=0, keepdims=True)
    s[:, pl.ds(WIDE, 128)] = jnp.zeros((8, 128), jnp.float32)
    for d in range(N):
        base = (PIECE * d) // 128 * 128
        both = s[:, pl.ds(base, 256)]
        shift = (256 - (PIECE * d - base)) % 256
        piece_a[d] = (pltpu.roll(both, shift, 1) if shift else both)[:, :128]
    pl.semaphore_wait(barrier, N - 1 + bank)

    def rs_copy(k, piece, part, which):
        to = peer(k)
        return remote(piece.at[to], part.at[me], rs_send.at[which, k], rs_recv.at[which, k], (bank, to))

    def rz_copy(k):
        return remote(router_part, router_line.at[:, column], rz_send.at[k], rz_recv.at[k], (bank, peer(k)))

    for k in ORDER:
        rs_copy(k, piece_a, part_a, 0).start()

    part_a[me] = piece_a[me]

    eye = lax.broadcasted_iota(jnp.int32, (PIECE, OWN), 0) == lax.broadcasted_iota(jnp.int32, (PIECE, OWN), 1)
    for m in range(8, 12):
        loads[m].wait()

    @pl.loop(0, N)
    def _(d):
        rows = pl.ds(pl.multiple_of(d * PIECE, 8), PIECE)
        for e in range(EXP):
            total = jnp.sum(jnp.abs(t[8 + e, rows, :]), axis=1, keepdims=True)
            piece_b[d, pl.ds(e, 1), :] = jnp.sum(jnp.where(eye, total, 0.0), axis=0, keepdims=True)
        piece_b[d, pl.ds(4, 4), :] = jnp.zeros((4, OWN), jnp.float32)

    for c in small_loads:
        c.wait()
    router_part[...] = (weight[...] * gain[...]).astype(jnp.bfloat16)
    router_line[:, column] = router_part[...]
    for k in ORDER:
        rs_copy(k, piece_b, part_b, 1).start()
    for k in ORDER:
        rz_copy(k).start()

    part_b[me] = piece_b[me]

    def turn(lo, hi):
        for m in range(lo, hi):
            for c in range(WIDE // 128):
                t[m, pl.ds(c * 128, 128), :] = x[m, :, pl.ds(c * 128, 128)].T

    def ag_copy(k, mine, whole, which):
        return remote(mine, whole.at[me], ag_send.at[which, k], ag_recv.at[which, k], (bank, peer(k)))

    def reduce_and_spread(piece, part, mine, whole, which):
        @pl.loop(1, N)
        def _(k):
            rs_copy(k, piece, part, which).wait_recv()

        total = part[0]
        for d in range(1, N):
            total = total + part[d]
        scale = total / D_MODEL
        mine[...] = scale
        whole[me] = scale

        for k in ORDER:
            ag_copy(k, mine, whole, which).start()

        return scale

    turn(0, 4)
    scale_a = reduce_and_spread(piece_a, part_a, mine_a, all_a, 0)
    scales_ab[...] = scale_a
    scale_b = reduce_and_spread(piece_b, part_b, mine_b, all_b, 1)
    scales_c[...] = scale_b

    @pl.loop(1, N)
    def _(j):
        @pl.when(bank >= j)
        def _():
            pl.semaphore_signal(later, inc=1, device_id=(bank - j, me), device_id_type=MESH)

    turn(4, 8)

    @pl.loop(1, N)
    def _(k):
        ag_copy(k, mine_a, all_a, 0).wait_recv()
        ag_copy(k, mine_b, all_b, 1).wait_recv()

    outs = (out_gate, out_up, out_down)

    def scaled(to, m):
        row = (all_a if m < 8 else all_b)[to, pl.ds(m % 8, 1), :]
        factor = jnp.sum(jnp.where(eye, 1.0 / row, 0.0), axis=1, keepdims=True)
        rows = pl.ds(pl.multiple_of(to * PIECE, 8), PIECE)
        return (t[m, rows, :] * factor).astype(jnp.bfloat16)

    def out_copy(k, i):
        return remote(
            send.at[k, pl.ds(4 * i, 4)], outs[i].at[:, :, column], out_send.at[i, k], out_recv.at[i, k], (bank, peer(k))
        )

    for k in ORDER:
        to = peer(k)
        for i in range(3):
            for e in range(EXP):
                send[k, 4 * i + e] = scaled(to, 4 * i + e)
            out_copy(k, i).start()

    @pl.loop(1, N)
    def _(k):
        rz_copy(k).wait_recv()

    def rb_copy(k):
        return remote(router_line, router_rows.at[bank], rb_send.at[k], rb_recv.at[k], (bank_peer(k), me))

    @pl.when(bank < N - 1)
    def _():
        pl.semaphore_wait(later, N - 1 - bank)

    @pl.loop(1, N)
    def _(k):
        rb_copy(k).start()

    router_rows[bank] = router_line[...]

    for m in range(12):
        outs[m // 4][m % 4, :, column] = scaled(me, m)

    @pl.loop(1, N)
    def _(k):
        for i in range(3):
            out_copy(k, i).wait()
        rb_copy(k).wait()
        rz_copy(k).wait_send()
        for which, (piece, part, mine, whole) in enumerate(
            ((piece_a, part_a, mine_a, all_a), (piece_b, part_b, mine_b, all_b))
        ):
            rs_copy(k, piece, part, which).wait_send()
            ag_copy(k, mine, whole, which).wait_send()


def exchange(gate, up, down, weight, gain):
    f32, bf16 = jnp.float32, jnp.bfloat16
    vmem, anywhere = pl.BlockSpec(memory_space=pltpu.VMEM), pl.BlockSpec(memory_space=pl.ANY)
    big = jax.ShapeDtypeStruct((EXP, PIECE, D_MODEL), bf16)
    small = jax.ShapeDtypeStruct((8, 128), f32)
    return pl.pallas_call(
        exchange_kernel,
        name="exchange",
        out_shape=(big, big, big, small, small, jax.ShapeDtypeStruct((N, EXP, D_MODEL), bf16)),
        in_specs=[anywhere] * 5,
        out_specs=(vmem,) * 6,
        scratch_shapes=[
            pltpu.VMEM((8, OWN, WIDE), f32),
            pltpu.VMEM((12, WIDE, OWN), f32),
            pltpu.VMEM((8, WIDE + 128), f32),
            pltpu.VMEM((N, 8, 128), f32),
            pltpu.VMEM((N, 8, 128), f32),
            pltpu.VMEM((N, 8, 128), f32),
            pltpu.VMEM((N, 8, 128), f32),
            pltpu.VMEM((8, 128), f32),
            pltpu.VMEM((8, 128), f32),
            pltpu.VMEM((N, 8, 128), f32),
            pltpu.VMEM((N, 8, 128), f32),
            pltpu.VMEM((N, 12, PIECE, OWN), bf16),
            pltpu.VMEM((EXP, OWN), bf16),
            pltpu.VMEM((EXP, D_MODEL), bf16),
            pltpu.VMEM((EXP, OWN), f32),
            pltpu.VMEM((1, OWN), f32),
            pltpu.SemaphoreType.DMA((14,)),
            pltpu.SemaphoreType.DMA((2, N)),
            pltpu.SemaphoreType.DMA((2, N)),
            pltpu.SemaphoreType.DMA((2, N)),
            pltpu.SemaphoreType.DMA((2, N)),
            pltpu.SemaphoreType.DMA((3, N)),
            pltpu.SemaphoreType.DMA((3, N)),
            pltpu.SemaphoreType.DMA((N,)),
            pltpu.SemaphoreType.DMA((N,)),
            pltpu.SemaphoreType.DMA((N,)),
            pltpu.SemaphoreType.DMA((N,)),
            pltpu.SemaphoreType.REGULAR,
        ],
        compiler_params=pltpu.CompilerParams(
            collective_id=0, has_side_effects=True, vmem_limit_bytes=48 * 1024 * 1024
        ),
    )(gate, up, down, weight, gain)


def finish_kernel(a, b, c, scales_ab, scales_c, rows, fa, fb, fc, sa, sb, sc, fr, router, sem):
    copies = [
        pltpu.make_async_copy(src, dst, sem.at[i]) for i, (src, dst) in enumerate(((a, fa), (b, fb), (c, fc)))
    ]
    for c_ in copies:
        c_.start()
    sa[...] = scales_ab[pl.ds(0, 4), pl.ds(0, PIECE)]
    sb[...] = scales_ab[pl.ds(4, 4), pl.ds(0, PIECE)]
    sc[...] = scales_c[pl.ds(0, 4), pl.ds(0, PIECE)]
    for i in range(N):
        router[pl.ds(4 * i, 4), :] = rows[i]
    last = pltpu.make_async_copy(router, fr, sem.at[3])
    last.start()
    for c_ in copies:
        c_.wait()
    last.wait()


def finish(*parts):
    f32, bf16 = jnp.float32, jnp.bfloat16
    vmem, anywhere = pl.BlockSpec(memory_space=pltpu.VMEM), pl.BlockSpec(memory_space=pl.ANY)
    big = jax.ShapeDtypeStruct((EXP, PIECE, D_MODEL), bf16)
    small = jax.ShapeDtypeStruct((EXP, PIECE), f32)
    return pl.pallas_call(
        finish_kernel,
        name="finish",
        out_shape=(big, big, big, small, small, small, jax.ShapeDtypeStruct((N * EXP, D_MODEL), bf16)),
        in_specs=[vmem] * 6,
        out_specs=(anywhere,) * 3 + (vmem,) * 3 + (anywhere,),
        scratch_shapes=[pltpu.VMEM((N * EXP, D_MODEL), bf16), pltpu.SemaphoreType.DMA((4,))],
        compiler_params=pltpu.CompilerParams(vmem_limit_bytes=16 * 1024 * 1024),
    )(*parts)


def local(master_gate, master_up, master_down, router_weight, router_gain):
    parts = exchange(master_gate, master_up, master_down, router_weight.T, router_gain.reshape(1, OWN))
    fa, fb, fc, sa, sb, sc, fr = finish(*parts)
    return (fa.transpose(0, 2, 1), fb.transpose(0, 2, 1), fc, sa, sb, sc, fr.T)


def solution(mesh):
    placed = (
        P("bank", "zero", None),
        P("bank", "zero", None),
        P("bank", None, "zero"),
        P("zero", "bank"),
        P("zero"),
    )
    return jax.shard_map(
        local,
        mesh=mesh,
        in_specs=placed,
        out_specs=(
            P("bank", None, "zero"),
            P("bank", None, "zero"),
            P("bank", "zero", None),
            P("bank", "zero"),
            P("bank", "zero"),
            P("bank", "zero"),
            P(),
        ),
        check_vma=False,
    )
```

```python
import functools

import jax
import jax.numpy as jnp
from jax import lax
from jax.experimental import pallas as pl
from jax.experimental.pallas import tpu as pltpu
from jax.sharding import PartitionSpec as P

MESH = pl.DeviceIdType.MESH
N = 16
D_MODEL = 2048
EXP = 4
WIDE = 1408
OWN = 128
PIECE = WIDE // N
PEERS = ((1, 1), (3, 3), (1, 3), (3, 1), (1, 0), (3, 0), (0, 1), (0, 3), (1, 2), (3, 2), (2, 1), (2, 3), (2, 2), (0, 2), (2, 0))
RAW = 1
RAW_CUTS = (0, 40, 88)
ORDER = tuple(4 * a + b for a, b in PEERS)


def exchange_kernel(
    gate, up, down, weight_hbm, gain_hbm,
    out_gate, out_up, out_down, scales, router_rows,
    x, t, s, piece, part, mine, whole, send, router_part, router_line, weight, gain, raw_in,
    load_sem, rs_send, rs_recv, ag_send, ag_recv, out_send, out_recv, rz_send, rz_recv, rb_send, rb_recv,
    raw_send, raw_recv, later,
):
    me = lax.axis_index("zero")
    bank = lax.axis_index("bank")
    outs = (out_gate, out_up, out_down)
    column = pl.ds(pl.multiple_of(me * OWN, OWN), OWN)

    def peer(k):
        y, xx = me // 4, me % 4
        return ((y + k // 4) % 4) * 4 + (xx + k % 4) % 4

    def remote(src, dst, send_sem, recv_sem, to):
        return pltpu.make_async_remote_copy(
            src_ref=src, dst_ref=dst, send_sem=send_sem, recv_sem=recv_sem, device_id=to, device_id_type=MESH
        )

    loads = {}
    for m in range(12):
        source = (gate, up, down)[m // 4].at[m % 4]
        target = x.at[m] if m < 8 else t.at[m]
        loads[m] = pltpu.make_async_copy(source, target, load_sem.at[m])
    loads[12] = pltpu.make_async_copy(weight_hbm, weight, load_sem.at[12])
    loads[13] = pltpu.make_async_copy(gain_hbm, gain, load_sem.at[13])
    for c in loads.values():
        c.start()

    barrier = pltpu.get_barrier_semaphore()
    for k in ORDER:
        pl.semaphore_signal(barrier, inc=1, device_id=(bank, peer(k)), device_id_type=MESH)

    @pl.loop(1, N)
    def _(j):
        @pl.when(bank + j < N)
        def _():
            pl.semaphore_signal(barrier, inc=1, device_id=(bank + j, me), device_id_type=MESH)

    def rs_copy(k, i):
        to = peer(k)
        return remote(piece.at[i, to], part.at[i, me], rs_send.at[i, k], rs_recv.at[i, k], (bank, to))

    def ag_copy(k, i):
        return remote(mine.at[i], whole.at[i, me], ag_send.at[i, k], ag_recv.at[i, k], (bank, peer(k)))

    def raw_copy(k, e, half):
        to = peer(k)
        lo, hi = RAW_CUTS[half], RAW_CUTS[half + 1]
        return remote(
            t.at[8 + e, pl.ds(pl.multiple_of(to * PIECE + lo, 8), hi - lo), :],
            raw_in.at[k, pl.ds(e * PIECE + lo, hi - lo), :],
            raw_send.at[e, half, k], raw_recv.at[e, half, k], (bank, to),
        )

    def raw_spread(half):
        if half == 0:
            for e in range(RAW):
                loads[8 + e].wait()
        for e in range(RAW):
            if RAW_CUTS[half + 1] > RAW_CUTS[half]:
                for k in ORDER:
                    raw_copy(k, e, half).start()

    def rz_copy(k):
        return remote(router_part, router_line.at[:, column], rz_send.at[k], rz_recv.at[k], (bank, peer(k)))

    s[:, pl.ds(WIDE, 128)] = jnp.zeros((8, 128), jnp.float32)

    def lane_sums(i):
        for m in range(4 * i, 4 * i + 4):
            loads[m].wait()
            s[pl.ds(m, 1), pl.ds(0, WIDE)] = jnp.sum(jnp.abs(x[m]), axis=0, keepdims=True)
        for d in range(N):
            base = (PIECE * d) // 128 * 128
            both = s[:, pl.ds(base, 256)]
            shift = (256 - (PIECE * d - base)) % 256
            moved = pltpu.roll(both, shift, 1) if shift else both
            piece[i, d] = moved[4 * i : 4 * i + 4, :128]

    eye = lax.broadcasted_iota(jnp.int32, (PIECE, OWN), 0) == lax.broadcasted_iota(jnp.int32, (PIECE, OWN), 1)

    def row_sums():
        for m in range(8 + RAW, 12):
            loads[m].wait()

        @pl.loop(0, N)
        def _(d):
            rows = pl.ds(pl.multiple_of(d * PIECE, 8), PIECE)
            for e in range(EXP):
                total = jnp.sum(jnp.abs(t[8 + e, rows, :]), axis=1, keepdims=True)
                piece[2, d, pl.ds(e, 1), :] = jnp.sum(jnp.where(eye, total, 0.0), axis=0, keepdims=True)

    def rs_spread(i):
        for k in ORDER:
            rs_copy(k, i).start()
        part[i, me] = piece[i, me]

    lane_sums(0)
    lane_sums(1)
    pl.semaphore_wait(barrier, N - 1 + bank)
    rs_spread(0)
    rs_spread(1)
    raw_spread(0)
    row_sums()
    rs_spread(2)

    loads[12].wait()
    loads[13].wait()
    router_part[...] = (weight[...] * gain[...]).astype(jnp.bfloat16)
    router_line[:, column] = router_part[...]
    for k in ORDER:
        rz_copy(k).start()

    @pl.loop(1, N)
    def _(j):
        @pl.when(bank >= j)
        def _():
            pl.semaphore_signal(later, inc=1, device_id=(bank - j, me), device_id_type=MESH)

    def turn(i):
        for m in range(4 * i, 4 * i + 4):
            for c in range(WIDE // 128):
                t[m, pl.ds(c * 128, 128), :] = x[m, :, pl.ds(c * 128, 128)].T

    def reduce_and_spread(i):
        @pl.loop(1, N)
        def _(k):
            rs_copy(k, i).wait_recv()

        total = part[i, 0]
        for d in range(1, N):
            total = total + part[i, d]
        scale = total / D_MODEL
        mine[i] = scale
        whole[i, me] = scale
        scales[i] = scale
        for k in ORDER:
            ag_copy(k, i).start()

    def upright(row):
        return jnp.sum(jnp.where(eye, 1.0 / row, 0.0), axis=1, keepdims=True)

    def scaled(to, m):
        factor = upright(whole[m // 4, to, pl.ds(m % 4, 1), :])
        rows = pl.ds(pl.multiple_of(to * PIECE, 8), PIECE)
        return (t[m, rows, :] * factor).astype(jnp.bfloat16)

    def out_copy(k, i):
        lo = RAW if i == 2 else 0
        return remote(
            send.at[k, pl.ds(4 * i + lo, 4 - lo)], outs[i].at[pl.ds(lo, 4 - lo), :, column],
            out_send.at[i, k], out_recv.at[i, k], (bank, peer(k)),
        )

    def out_spread(i):
        @pl.loop(1, N)
        def _(k):
            ag_copy(k, i).wait_recv()

        for k in ORDER:
            to = peer(k)
            for e in range(RAW if i == 2 else 0, EXP):
                send[k, 4 * i + e] = scaled(to, 4 * i + e)
            out_copy(k, i).start()

    turn(0)
    reduce_and_spread(0)
    reduce_and_spread(1)
    raw_spread(1)
    reduce_and_spread(2)
    out_spread(0)
    turn(1)
    out_spread(1)
    out_spread(2)

    @pl.loop(1, N)
    def _(k):
        rz_copy(k).wait_recv()

    def rb_copy(k):
        return remote(
            router_line, router_rows.at[bank], rb_send.at[k], rb_recv.at[k], ((bank + k) % N, me)
        )

    @pl.when(bank < N - 1)
    def _():
        pl.semaphore_wait(later, N - 1 - bank)

    @pl.loop(1, N)
    def _(k):
        rb_copy(k).start()

    router_rows[bank] = router_line[...]
    for m in range(12):
        outs[m // 4][m % 4, :, column] = scaled(me, m)

    for e in range(RAW):
        factor = upright(mine[2, pl.ds(e, 1), :])

        @pl.loop(1, N)
        def _(k):
            for half in range(2):
                if RAW_CUTS[half + 1] > RAW_CUTS[half]:
                    raw_copy(k, e, half).wait_recv()
            source = ((me // 4 + 4 - k // 4) % 4) * 4 + (me % 4 + 4 - k % 4) % 4
            block = raw_in[k, pl.ds(e * PIECE, PIECE), :] * factor
            out_down[e, :, pl.ds(pl.multiple_of(source * OWN, OWN), OWN)] = block.astype(jnp.bfloat16)

    @pl.loop(1, N)
    def _(k):
        for i in range(3):
            out_copy(k, i).wait()
            rs_copy(k, i).wait_send()
            ag_copy(k, i).wait_send()
        rb_copy(k).wait()
        rz_copy(k).wait_send()
        for e in range(RAW):
            for half in range(2):
                if RAW_CUTS[half + 1] > RAW_CUTS[half]:
                    raw_copy(k, e, half).wait_send()


def exchange(gate, up, down, weight, gain):
    f32, bf16 = jnp.float32, jnp.bfloat16
    vmem, anywhere = pl.BlockSpec(memory_space=pltpu.VMEM), pl.BlockSpec(memory_space=pl.ANY)
    big = jax.ShapeDtypeStruct((EXP, PIECE, D_MODEL), bf16)
    return pl.pallas_call(
        exchange_kernel,
        name="exchange",
        out_shape=(big, big, big, jax.ShapeDtypeStruct((3, EXP, 128), f32), jax.ShapeDtypeStruct((N, EXP, D_MODEL), bf16)),
        in_specs=[anywhere] * 5,
        out_specs=(vmem,) * 5,
        scratch_shapes=[
            pltpu.VMEM((8, OWN, WIDE), f32),
            pltpu.VMEM((12, WIDE, OWN), f32),
            pltpu.VMEM((8, WIDE + 128), f32),
            pltpu.VMEM((3, N, EXP, 128), f32),
            pltpu.VMEM((3, N, EXP, 128), f32),
            pltpu.VMEM((3, EXP, 128), f32),
            pltpu.VMEM((3, N, EXP, 128), f32),
            pltpu.VMEM((N, 12, PIECE, OWN), bf16),
            pltpu.VMEM((EXP, OWN), bf16),
            pltpu.VMEM((EXP, D_MODEL), bf16),
            pltpu.VMEM((EXP, OWN), f32),
            pltpu.VMEM((1, OWN), f32),
            pltpu.VMEM((N, max(RAW, 1) * PIECE, OWN), f32),
            pltpu.SemaphoreType.DMA((14,)),
        ]
        + [pltpu.SemaphoreType.DMA((3, N))] * 6
        + [pltpu.SemaphoreType.DMA((N,))] * 4
        + [pltpu.SemaphoreType.DMA((max(RAW, 1), 2, N))] * 2
        + [pltpu.SemaphoreType.REGULAR],
        compiler_params=pltpu.CompilerParams(
            collective_id=0, has_side_effects=True, vmem_limit_bytes=48 * 1024 * 1024
        ),
    )(gate, up, down, weight, gain)


def finish_kernel(a, b, c, scales, rows, fa, fb, fc, sa, sb, sc, fr, router, sem):
    copies = [
        pltpu.make_async_copy(src, dst, sem.at[i]) for i, (src, dst) in enumerate(((a, fa), (b, fb), (c, fc)))
    ]
    for c_ in copies:
        c_.start()
    sa[...] = scales[0, :, pl.ds(0, PIECE)]
    sb[...] = scales[1, :, pl.ds(0, PIECE)]
    sc[...] = scales[2, :, pl.ds(0, PIECE)]
    for i in range(N):
        router[pl.ds(4 * i, 4), :] = rows[i]
    last = pltpu.make_async_copy(router, fr, sem.at[3])
    last.start()
    for c_ in copies:
        c_.wait()
    last.wait()


def finish(*parts):
    f32, bf16 = jnp.float32, jnp.bfloat16
    vmem, anywhere = pl.BlockSpec(memory_space=pltpu.VMEM), pl.BlockSpec(memory_space=pl.ANY)
    big = jax.ShapeDtypeStruct((EXP, PIECE, D_MODEL), bf16)
    small = jax.ShapeDtypeStruct((EXP, PIECE), f32)
    return pl.pallas_call(
        finish_kernel,
        name="finish",
        out_shape=(big, big, big, small, small, small, jax.ShapeDtypeStruct((N * EXP, D_MODEL), bf16)),
        in_specs=[vmem] * 5,
        out_specs=(anywhere,) * 3 + (vmem,) * 3 + (anywhere,),
        scratch_shapes=[pltpu.VMEM((N * EXP, D_MODEL), bf16), pltpu.SemaphoreType.DMA((4,))],
        compiler_params=pltpu.CompilerParams(vmem_limit_bytes=16 * 1024 * 1024),
    )(*parts)


def local(master_gate, master_up, master_down, router_weight, router_gain):
    parts = exchange(master_gate, master_up, master_down, router_weight.T, router_gain.reshape(1, OWN))
    fa, fb, fc, sa, sb, sc, fr = finish(*parts)
    return (fa.transpose(0, 2, 1), fb.transpose(0, 2, 1), fc, sa, sb, sc, fr.T)


def solution(mesh):
    placed = (
        P("bank", "zero", None),
        P("bank", "zero", None),
        P("bank", None, "zero"),
        P("zero", "bank"),
        P("zero"),
    )
    return jax.shard_map(
        local,
        mesh=mesh,
        in_specs=placed,
        out_specs=(
            P("bank", None, "zero"),
            P("bank", None, "zero"),
            P("bank", "zero", None),
            P("bank", "zero"),
            P("bank", "zero"),
            P("bank", "zero"),
            P(),
        ),
        check_vma=False,
    )
```

```python
import functools

import jax
import jax.numpy as jnp
from jax import lax
from jax.experimental import pallas as pl
from jax.experimental.pallas import tpu as pltpu
from jax.sharding import PartitionSpec as P

MESH = pl.DeviceIdType.MESH
N = 16
D_MODEL = 2048
EXP = 4
WIDE = 1408
OWN = 128
PIECE = WIDE // N
PEERS = ((1, 1), (3, 3), (1, 3), (3, 1), (1, 0), (3, 0), (0, 1), (0, 3), (1, 2), (3, 2), (2, 1), (2, 3), (2, 2), (0, 2), (2, 0))
RAW_CUTS = (0, 40, 64)
RAW_END = RAW_CUTS[2]
ORDER = tuple(4 * a + b for a, b in PEERS)
FAR_FIRST = ORDER
LAST_ORDER = ORDER


def exchange_kernel(
    gate, up, down, weight_hbm, gain_hbm,
    out_gate, out_up, out_down, scale_gate, scale_up, scale_down, router,
    router_rows, x, t, s, piece, part, mine, whole, send, router_part, router_line, weight, gain, raw_in,
    load_sem, rs_send, rs_recv, ag_send, ag_recv, out_send, out_recv, rz_send, rz_recv, rb_send, rb_recv,
    raw_send, raw_recv, later,
):
    me = lax.axis_index("zero")
    bank = lax.axis_index("bank")
    outs, scales = (out_gate, out_up, out_down), (scale_gate, scale_up, scale_down)
    column = pl.ds(pl.multiple_of(me * OWN, OWN), OWN)

    def peer(k):
        y, xx = me // 4, me % 4
        return ((y + k // 4) % 4) * 4 + (xx + k % 4) % 4

    def remote(src, dst, send_sem, recv_sem, to):
        return pltpu.make_async_remote_copy(
            src_ref=src, dst_ref=dst, send_sem=send_sem, recv_sem=recv_sem, device_id=to, device_id_type=MESH
        )

    loads = {}
    for m in range(12):
        source = (gate, up, down)[m // 4].at[m % 4]
        target = x.at[m] if m < 8 else t.at[m]
        loads[m] = pltpu.make_async_copy(source, target, load_sem.at[m])
    loads[12] = pltpu.make_async_copy(weight_hbm, weight, load_sem.at[12])
    loads[13] = pltpu.make_async_copy(gain_hbm, gain, load_sem.at[13])
    for c in loads.values():
        c.start()

    barrier = pltpu.get_barrier_semaphore()
    for k in ORDER:
        pl.semaphore_signal(barrier, inc=1, device_id=(bank, peer(k)), device_id_type=MESH)

    @pl.loop(1, N)
    def _(j):
        @pl.when(bank + j < N)
        def _():
            pl.semaphore_signal(barrier, inc=1, device_id=(bank + j, me), device_id_type=MESH)

    def rs_copy(k, i):
        to = peer(k)
        return remote(piece.at[i, to], part.at[i, me], rs_send.at[i, k], rs_recv.at[i, k], (bank, to))

    def ag_copy(k, i):
        return remote(mine.at[i], whole.at[i, me], ag_send.at[i, k], ag_recv.at[i, k], (bank, peer(k)))

    halves = [h for h in range(2) if RAW_CUTS[h + 1] > RAW_CUTS[h]]

    def raw_copy(k, half):
        to = peer(k)
        lo, hi = RAW_CUTS[half], RAW_CUTS[half + 1]
        return remote(
            t.at[8, pl.ds(pl.multiple_of(to * PIECE + lo, 8), hi - lo), :], raw_in.at[k, pl.ds(lo, hi - lo), :],
            raw_send.at[half, k], raw_recv.at[half, k], (bank, to),
        )

    def raw_spread(half):
        if half in halves:
            for k in ORDER:
                raw_copy(k, half).start()

    def rz_copy(k):
        return remote(router_part, router_line.at[:, column], rz_send.at[k], rz_recv.at[k], (bank, peer(k)))

    s[:, pl.ds(WIDE, 128)] = jnp.zeros((8, 128), jnp.float32)

    def lane_sums(i):
        for m in range(4 * i, 4 * i + 4):
            loads[m].wait()
            s[pl.ds(m, 1), pl.ds(0, WIDE)] = jnp.sum(jnp.abs(x[m]), axis=0, keepdims=True)
        for d in range(N):
            base = (PIECE * d) // 128 * 128
            both = s[:, pl.ds(base, 256)]
            shift = (256 - (PIECE * d - base)) % 256
            moved = pltpu.roll(both, shift, 1) if shift else both
            piece[i, d] = moved[4 * i : 4 * i + 4, :128]

    eye = lax.broadcasted_iota(jnp.int32, (PIECE, OWN), 0) == lax.broadcasted_iota(jnp.int32, (PIECE, OWN), 1)

    def row_sums():
        for m in range(9, 12):
            loads[m].wait()

        @pl.loop(0, N)
        def _(d):
            rows = pl.ds(pl.multiple_of(d * PIECE, 8), PIECE)
            for e in range(EXP):
                total = jnp.sum(jnp.abs(t[8 + e, rows, :]), axis=1, keepdims=True)
                piece[2, d, pl.ds(e, 1), :] = jnp.sum(jnp.where(eye, total, 0.0), axis=0, keepdims=True)

    def rs_spread(i):
        for k in FAR_FIRST:
            rs_copy(k, i).start()
        part[i, me] = piece[i, me]

    lane_sums(0)
    lane_sums(1)
    pl.semaphore_wait(barrier, N - 1 + bank)
    rs_spread(0)
    rs_spread(1)
    loads[8].wait()
    raw_spread(0)
    row_sums()
    rs_spread(2)

    loads[12].wait()
    loads[13].wait()
    router_part[...] = (weight[...] * gain[...]).astype(jnp.bfloat16)
    router_line[:, column] = router_part[...]
    for k in ORDER:
        rz_copy(k).start()

    @pl.loop(1, N)
    def _(j):
        @pl.when(bank >= j)
        def _():
            pl.semaphore_signal(later, inc=1, device_id=(bank - j, me), device_id_type=MESH)

    def turn(i):
        for m in range(4 * i, 4 * i + 4):
            for c in range(WIDE // 128):
                t[m, pl.ds(c * 128, 128), :] = x[m, :, pl.ds(c * 128, 128)].T

    def reduce_and_spread(i):
        @pl.loop(1, N)
        def _(k):
            rs_copy(k, i).wait_recv()

        total = part[i, 0]
        for d in range(1, N):
            total = total + part[i, d]
        scale = total / D_MODEL
        mine[i] = scale
        whole[i, me] = scale
        scales[i][...] = scale[:, :PIECE]
        for k in FAR_FIRST:
            ag_copy(k, i).start()

    def upright(row):
        return jnp.sum(jnp.where(eye, 1.0 / row, 0.0), axis=1, keepdims=True)

    def scaled(to, m, lo=0):
        factor = upright(whole[m // 4, to, pl.ds(m % 4, 1), :])[lo:]
        rows = pl.ds(pl.multiple_of(to * PIECE + lo, 8), PIECE - lo)
        return (t[m, rows, :] * factor).astype(jnp.bfloat16)

    def out_copies(k, i):
        first = 1 if i == 2 and RAW_END else 0
        copies = [
            remote(
                send.at[k, pl.ds(4 * i + first, 4 - first)], outs[i].at[pl.ds(first, 4 - first), :, column],
                out_send.at[i, k], out_recv.at[i, k], (bank, peer(k)),
            )
        ]
        if first and RAW_END < PIECE:
            rest = pl.ds(RAW_END, PIECE - RAW_END)
            copies.append(
                remote(
                    send.at[k, 8, rest, :], out_down.at[0, rest, column],
                    out_send.at[3, k], out_recv.at[3, k], (bank, peer(k)),
                )
            )
        return copies

    def out_spread(i):
        for k in LAST_ORDER if i == 2 else ORDER:
            to = peer(k)
            back = (4 - k // 4) % 4 * 4 + (4 - k % 4) % 4
            ag_copy(back, i).wait_recv()
            for e in range(EXP):
                lo = RAW_END if i == 2 and e == 0 else 0
                if lo < PIECE:
                    send[k, 4 * i + e, pl.ds(lo, PIECE - lo), :] = scaled(to, 4 * i + e, lo)
            for c in out_copies(k, i):
                c.start()

    turn(0)
    reduce_and_spread(0)
    reduce_and_spread(1)
    raw_spread(1)
    reduce_and_spread(2)
    out_spread(0)
    turn(1)
    out_spread(1)
    out_spread(2)

    @pl.loop(1, N)
    def _(k):
        rz_copy(k).wait_recv()

    def rb_copy(k):
        return remote(
            router_line, router_rows.at[bank], rb_send.at[k], rb_recv.at[k], ((bank + k) % N, me)
        )

    @pl.when(bank < N - 1)
    def _():
        pl.semaphore_wait(later, N - 1 - bank)

    @pl.loop(1, N)
    def _(k):
        rb_copy(k).start()

    router_rows[bank] = router_line[...]
    for m in range(12):
        outs[m // 4][m % 4, :, column] = scaled(me, m)

    if RAW_END:
        own = upright(mine[2, pl.ds(0, 1), :])[:RAW_END]

        @pl.loop(1, N)
        def _(k):
            for half in halves:
                raw_copy(k, half).wait_recv()
            source = ((me // 4 + 4 - k // 4) % 4) * 4 + (me % 4 + 4 - k % 4) % 4
            block = raw_in[k, pl.ds(0, RAW_END), :] * own
            out_down[0, pl.ds(0, RAW_END), pl.ds(pl.multiple_of(source * OWN, OWN), OWN)] = block.astype(jnp.bfloat16)

    @pl.loop(1, N)
    def _(k):
        rb_copy(k).wait()

    for b in range(N):
        router[pl.ds(EXP * b, EXP), :] = router_rows[b]

    @pl.loop(1, N)
    def _(k):
        for i in range(3):
            rs_copy(k, i).wait_send()
            ag_copy(k, i).wait_send()
            for c in out_copies(k, i):
                c.wait()
        rz_copy(k).wait_send()
        for half in halves:
            raw_copy(k, half).wait_send()


def exchange(gate, up, down, weight, gain):
    f32, bf16 = jnp.float32, jnp.bfloat16
    vmem = pl.BlockSpec(memory_space=pltpu.VMEM)
    big = jax.ShapeDtypeStruct((EXP, PIECE, D_MODEL), bf16)
    small = jax.ShapeDtypeStruct((EXP, PIECE), f32)
    return pl.pallas_call(
        exchange_kernel,
        name="exchange",
        out_shape=(big, big, big, small, small, small, jax.ShapeDtypeStruct((N * EXP, D_MODEL), bf16)),
        in_specs=[pl.BlockSpec(memory_space=pltpu.HBM)] * 5,
        out_specs=(vmem,) * 7,
        scratch_shapes=[
            pltpu.VMEM((N, EXP, D_MODEL), bf16),
            pltpu.VMEM((8, OWN, WIDE), f32),
            pltpu.VMEM((12, WIDE, OWN), f32),
            pltpu.VMEM((8, WIDE + 128), f32),
            pltpu.VMEM((3, N, EXP, 128), f32),
            pltpu.VMEM((3, N, EXP, 128), f32),
            pltpu.VMEM((3, EXP, 128), f32),
            pltpu.VMEM((3, N, EXP, 128), f32),
            pltpu.VMEM((N, 12, PIECE, OWN), bf16),
            pltpu.VMEM((EXP, OWN), bf16),
            pltpu.VMEM((EXP, D_MODEL), bf16),
            pltpu.VMEM((EXP, OWN), f32),
            pltpu.VMEM((1, OWN), f32),
            pltpu.VMEM((N, PIECE, OWN), f32),
            pltpu.SemaphoreType.DMA((14,)),
        ]
        + [pltpu.SemaphoreType.DMA((3, N))] * 4
        + [pltpu.SemaphoreType.DMA((4, N))] * 2
        + [pltpu.SemaphoreType.DMA((N,))] * 4
        + [pltpu.SemaphoreType.DMA((2, N))] * 2
        + [pltpu.SemaphoreType.REGULAR],
        compiler_params=pltpu.CompilerParams(
            collective_id=0, has_side_effects=True, vmem_limit_bytes=48 * 1024 * 1024
        ),
    )(gate, up, down, weight, gain)


def finish_kernel(*refs):
    sem = refs[-1]
    copies = [pltpu.make_async_copy(refs[i], refs[7 + i], sem.at[i]) for i in range(7)]
    for c in copies:
        c.start()
    for c in copies:
        c.wait()


def finish(*parts):
    vmem, anywhere = pl.BlockSpec(memory_space=pltpu.VMEM), pl.BlockSpec(memory_space=pl.ANY)
    return pl.pallas_call(
        finish_kernel,
        name="finish",
        out_shape=tuple(jax.ShapeDtypeStruct(p.shape, p.dtype) for p in parts),
        in_specs=[vmem] * 7,
        out_specs=(anywhere,) * 7,
        scratch_shapes=[pltpu.SemaphoreType.DMA((7,))],
        compiler_params=pltpu.CompilerParams(vmem_limit_bytes=16 * 1024 * 1024),
    )(*parts)


def local(master_gate, master_up, master_down, router_weight, router_gain):
    router_weight, router_gain = (
        pltpu.with_memory_space_constraint(a, pltpu.HBM) for a in (router_weight.T, router_gain.reshape(1, OWN))
    )
    parts = exchange(master_gate, master_up, master_down, router_weight, router_gain)
    fa, fb, fc, sa, sb, sc, fr = finish(*parts)
    return (fa.transpose(0, 2, 1), fb.transpose(0, 2, 1), fc, sa, sb, sc, fr.T)


def solution(mesh):
    placed = (
        P("bank", "zero", None),
        P("bank", "zero", None),
        P("bank", None, "zero"),
        P("zero", "bank"),
        P("zero"),
    )
    return jax.shard_map(
        local,
        mesh=mesh,
        in_specs=placed,
        out_specs=(
            P("bank", None, "zero"),
            P("bank", None, "zero"),
            P("bank", "zero", None),
            P("bank", "zero"),
            P("bank", "zero"),
            P("bank", "zero"),
            P(),
        ),
        check_vma=False,
    )
```

```python
import functools

import jax
import jax.numpy as jnp
from jax import lax
from jax.experimental import pallas as pl
from jax.experimental.pallas import tpu as pltpu
from jax.sharding import PartitionSpec as P

MESH = pl.DeviceIdType.MESH
N = 16
D_MODEL = 2048
EXP = 4
WIDE = 1408
OWN = 128
PIECE = WIDE // N
PEERS = ((1, 1), (3, 3), (1, 3), (3, 1), (1, 0), (3, 0), (0, 1), (0, 3), (1, 2), (3, 2), (2, 1), (2, 3), (2, 2), (0, 2), (2, 0))
RAW_CUTS = (0, 40, 64)
RAW_END = RAW_CUTS[2]
ORDER = tuple(4 * a + b for a, b in PEERS)
FAR_FIRST = ORDER
LAST_ORDER = ORDER


def exchange_kernel(
    gate, up, down, weight_hbm, gain_hbm,
    out_gate, out_up, out_down, scale_gate, scale_up, scale_down, router,
    router_rows, x, t, s, piece, part, mine, whole, send, router_part, router_line, weight, gain, raw_in,
    load_sem, rs_send, rs_recv, ag_send, ag_recv, out_send, out_recv, rz_send, rz_recv, rb_send, rb_recv,
    raw_send, raw_recv, later,
):
    me = lax.axis_index("zero")
    bank = lax.axis_index("bank")
    outs, scales = (out_gate, out_up, out_down), (scale_gate, scale_up, scale_down)
    column = pl.ds(pl.multiple_of(me * OWN, OWN), OWN)

    def peer(k):
        y, xx = me // 4, me % 4
        return ((y + k // 4) % 4) * 4 + (xx + k % 4) % 4

    def remote(src, dst, send_sem, recv_sem, to):
        return pltpu.make_async_remote_copy(
            src_ref=src, dst_ref=dst, send_sem=send_sem, recv_sem=recv_sem, device_id=to, device_id_type=MESH
        )

    loads = {}
    for m in range(12):
        source = (gate, up, down)[m // 4].at[m % 4]
        target = x.at[m] if m < 8 else t.at[m]
        loads[m] = pltpu.make_async_copy(source, target, load_sem.at[m])
    loads[12] = pltpu.make_async_copy(weight_hbm, weight, load_sem.at[12])
    loads[13] = pltpu.make_async_copy(gain_hbm, gain, load_sem.at[13])
    for c in loads.values():
        c.start()

    barrier = pltpu.get_barrier_semaphore()
    for k in ORDER:
        pl.semaphore_signal(barrier, inc=1, device_id=(bank, peer(k)), device_id_type=MESH)

    @pl.loop(1, N)
    def _(j):
        @pl.when(bank + j < N)
        def _():
            pl.semaphore_signal(barrier, inc=1, device_id=(bank + j, me), device_id_type=MESH)

    def rs_copy(k, i):
        to = peer(k)
        return remote(piece.at[i, to], part.at[i, me], rs_send.at[i, k], rs_recv.at[i, k], (bank, to))

    def ag_copy(k, i):
        return remote(mine.at[i], whole.at[i, me], ag_send.at[i, k], ag_recv.at[i, k], (bank, peer(k)))

    halves = [h for h in range(2) if RAW_CUTS[h + 1] > RAW_CUTS[h]]

    def raw_copy(k, half):
        to = peer(k)
        lo, hi = RAW_CUTS[half], RAW_CUTS[half + 1]
        return remote(
            t.at[8, pl.ds(pl.multiple_of(to * PIECE + lo, 8), hi - lo), :], raw_in.at[k, pl.ds(lo, hi - lo), :],
            raw_send.at[half, k], raw_recv.at[half, k], (bank, to),
        )

    def raw_spread(half):
        if half in halves:
            for k in ORDER:
                raw_copy(k, half).start()

    def rz_copy(k):
        return remote(router_part, router_line.at[:, column], rz_send.at[k], rz_recv.at[k], (bank, peer(k)))

    s[:, pl.ds(WIDE, 128)] = jnp.zeros((8, 128), jnp.float32)

    def lane_sums(i):
        for m in range(4 * i, 4 * i + 4):
            loads[m].wait()
            s[pl.ds(m, 1), pl.ds(0, WIDE)] = jnp.sum(jnp.abs(x[m]), axis=0, keepdims=True)
        for d in range(N):
            base = (PIECE * d) // 128 * 128
            both = s[:, pl.ds(base, 256)]
            shift = (256 - (PIECE * d - base)) % 256
            moved = pltpu.roll(both, shift, 1) if shift else both
            piece[i, d] = moved[4 * i : 4 * i + 4, :128]

    eye = lax.broadcasted_iota(jnp.int32, (PIECE, OWN), 0) == lax.broadcasted_iota(jnp.int32, (PIECE, OWN), 1)

    def row_sums():
        for m in range(9, 12):
            loads[m].wait()

        @pl.loop(0, N)
        def _(d):
            rows = pl.ds(pl.multiple_of(d * PIECE, 8), PIECE)
            for e in range(EXP):
                total = jnp.sum(jnp.abs(t[8 + e, rows, :]), axis=1, keepdims=True)
                piece[2, d, pl.ds(e, 1), :] = jnp.sum(jnp.where(eye, total, 0.0), axis=0, keepdims=True)

    def rs_spread(i):
        for k in FAR_FIRST:
            rs_copy(k, i).start()
        part[i, me] = piece[i, me]

    lane_sums(0)
    lane_sums(1)
    pl.semaphore_wait(barrier, N - 1 + bank)
    rs_spread(0)
    rs_spread(1)
    loads[8].wait()
    raw_spread(0)
    row_sums()
    rs_spread(2)

    loads[12].wait()
    loads[13].wait()
    router_part[...] = (weight[...] * gain[...]).astype(jnp.bfloat16)
    router_line[:, column] = router_part[...]
    for k in ORDER:
        rz_copy(k).start()

    @pl.loop(1, N)
    def _(j):
        @pl.when(bank >= j)
        def _():
            pl.semaphore_signal(later, inc=1, device_id=(bank - j, me), device_id_type=MESH)

    def turn(i):
        for m in range(4 * i, 4 * i + 4):
            for c in range(WIDE // 128):
                t[m, pl.ds(c * 128, 128), :] = x[m, :, pl.ds(c * 128, 128)].T

    def reduce_and_spread(i):
        @pl.loop(1, N)
        def _(k):
            rs_copy(k, i).wait_recv()

        total = part[i, 0]
        for d in range(1, N):
            total = total + part[i, d]
        scale = total / D_MODEL
        mine[i] = scale
        whole[i, me] = scale
        scales[i][...] = scale[:, :PIECE]
        for k in FAR_FIRST:
            ag_copy(k, i).start()

    def upright(row):
        return jnp.sum(jnp.where(eye, 1.0 / row, 0.0), axis=1, keepdims=True)

    def scaled(to, m, lo=0):
        factor = upright(whole[m // 4, to, pl.ds(m % 4, 1), :])[lo:]
        rows = pl.ds(pl.multiple_of(to * PIECE + lo, 8), PIECE - lo)
        return (t[m, rows, :] * factor).astype(jnp.bfloat16)

    def out_copies(k, i):
        first = 1 if i == 2 and RAW_END else 0
        copies = [
            remote(
                send.at[k, pl.ds(4 * i + first, 4 - first)], outs[i].at[pl.ds(first, 4 - first), :, column],
                out_send.at[i, k], out_recv.at[i, k], (bank, peer(k)),
            )
        ]
        if first and RAW_END < PIECE:
            rest = pl.ds(RAW_END, PIECE - RAW_END)
            copies.append(
                remote(
                    send.at[k, 8, rest, :], out_down.at[0, rest, column],
                    out_send.at[3, k], out_recv.at[3, k], (bank, peer(k)),
                )
            )
        return copies

    def out_spread(i):
        for k in LAST_ORDER if i == 2 else ORDER:
            to = peer(k)
            back = (4 - k // 4) % 4 * 4 + (4 - k % 4) % 4
            ag_copy(back, i).wait_recv()
            for e in range(EXP):
                lo = RAW_END if i == 2 and e == 0 else 0
                if lo < PIECE:
                    send[k, 4 * i + e, pl.ds(lo, PIECE - lo), :] = scaled(to, 4 * i + e, lo)
            for c in out_copies(k, i):
                c.start()

    turn(0)
    reduce_and_spread(0)
    reduce_and_spread(1)
    raw_spread(1)
    out_spread(0)
    reduce_and_spread(2)
    turn(1)
    out_spread(1)
    out_spread(2)

    @pl.loop(1, N)
    def _(k):
        rz_copy(k).wait_recv()

    def rb_copy(k):
        return remote(
            router_line, router_rows.at[bank], rb_send.at[k], rb_recv.at[k], ((bank + k) % N, me)
        )

    @pl.when(bank < N - 1)
    def _():
        pl.semaphore_wait(later, N - 1 - bank)

    @pl.loop(1, N)
    def _(k):
        rb_copy(k).start()

    router_rows[bank] = router_line[...]
    for m in range(12):
        outs[m // 4][m % 4, :, column] = scaled(me, m)

    if RAW_END:
        own = upright(mine[2, pl.ds(0, 1), :])[:RAW_END]

        @pl.loop(1, N)
        def _(k):
            for half in halves:
                raw_copy(k, half).wait_recv()
            source = ((me // 4 + 4 - k // 4) % 4) * 4 + (me % 4 + 4 - k % 4) % 4
            block = raw_in[k, pl.ds(0, RAW_END), :] * own
            out_down[0, pl.ds(0, RAW_END), pl.ds(pl.multiple_of(source * OWN, OWN), OWN)] = block.astype(jnp.bfloat16)

    @pl.loop(1, N)
    def _(k):
        rb_copy(k).wait()

    for b in range(N):
        router[pl.ds(EXP * b, EXP), :] = router_rows[b]

    @pl.loop(1, N)
    def _(k):
        for i in range(3):
            rs_copy(k, i).wait_send()
            ag_copy(k, i).wait_send()
            for c in out_copies(k, i):
                c.wait()
        rz_copy(k).wait_send()
        for half in halves:
            raw_copy(k, half).wait_send()


def exchange(gate, up, down, weight, gain):
    f32, bf16 = jnp.float32, jnp.bfloat16
    vmem = pl.BlockSpec(memory_space=pltpu.VMEM)
    big = jax.ShapeDtypeStruct((EXP, PIECE, D_MODEL), bf16)
    small = jax.ShapeDtypeStruct((EXP, PIECE), f32)
    return pl.pallas_call(
        exchange_kernel,
        name="exchange",
        out_shape=(big, big, big, small, small, small, jax.ShapeDtypeStruct((N * EXP, D_MODEL), bf16)),
        in_specs=[pl.BlockSpec(memory_space=pltpu.HBM)] * 5,
        out_specs=(vmem,) * 7,
        scratch_shapes=[
            pltpu.VMEM((N, EXP, D_MODEL), bf16),
            pltpu.VMEM((8, OWN, WIDE), f32),
            pltpu.VMEM((12, WIDE, OWN), f32),
            pltpu.VMEM((8, WIDE + 128), f32),
            pltpu.VMEM((3, N, EXP, 128), f32),
            pltpu.VMEM((3, N, EXP, 128), f32),
            pltpu.VMEM((3, EXP, 128), f32),
            pltpu.VMEM((3, N, EXP, 128), f32),
            pltpu.VMEM((N, 12, PIECE, OWN), bf16),
            pltpu.VMEM((EXP, OWN), bf16),
            pltpu.VMEM((EXP, D_MODEL), bf16),
            pltpu.VMEM((EXP, OWN), f32),
            pltpu.VMEM((1, OWN), f32),
            pltpu.VMEM((N, PIECE, OWN), f32),
            pltpu.SemaphoreType.DMA((14,)),
        ]
        + [pltpu.SemaphoreType.DMA((3, N))] * 4
        + [pltpu.SemaphoreType.DMA((4, N))] * 2
        + [pltpu.SemaphoreType.DMA((N,))] * 4
        + [pltpu.SemaphoreType.DMA((2, N))] * 2
        + [pltpu.SemaphoreType.REGULAR],
        compiler_params=pltpu.CompilerParams(
            collective_id=0, has_side_effects=True, vmem_limit_bytes=48 * 1024 * 1024
        ),
    )(gate, up, down, weight, gain)


def finish_kernel(*refs):
    sem = refs[-1]
    copies = [pltpu.make_async_copy(refs[i], refs[7 + i], sem.at[i]) for i in range(7)]
    for c in copies:
        c.start()
    for c in copies:
        c.wait()


def finish(*parts):
    vmem, anywhere = pl.BlockSpec(memory_space=pltpu.VMEM), pl.BlockSpec(memory_space=pl.ANY)
    return pl.pallas_call(
        finish_kernel,
        name="finish",
        out_shape=tuple(jax.ShapeDtypeStruct(p.shape, p.dtype) for p in parts),
        in_specs=[vmem] * 7,
        out_specs=(anywhere,) * 7,
        scratch_shapes=[pltpu.SemaphoreType.DMA((7,))],
        compiler_params=pltpu.CompilerParams(vmem_limit_bytes=16 * 1024 * 1024),
    )(*parts)


def local(master_gate, master_up, master_down, router_weight, router_gain):
    router_weight, router_gain = (
        pltpu.with_memory_space_constraint(a, pltpu.HBM) for a in (router_weight.T, router_gain.reshape(1, OWN))
    )
    parts = exchange(master_gate, master_up, master_down, router_weight, router_gain)
    fa, fb, fc, sa, sb, sc, fr = finish(*parts)
    return (fa.transpose(0, 2, 1), fb.transpose(0, 2, 1), fc, sa, sb, sc, fr.T)


def solution(mesh):
    placed = (
        P("bank", "zero", None),
        P("bank", "zero", None),
        P("bank", None, "zero"),
        P("zero", "bank"),
        P("zero"),
    )
    return jax.shard_map(
        local,
        mesh=mesh,
        in_specs=placed,
        out_specs=(
            P("bank", None, "zero"),
            P("bank", None, "zero"),
            P("bank", "zero", None),
            P("bank", "zero"),
            P("bank", "zero"),
            P("bank", "zero"),
            P(),
        ),
        check_vma=False,
    )
```
